32 devices in a mesh: row: 16 (over z, y, x), col: 2 (over core).
Axes of the slice: x: 2, y: 2, z: 4, core: 2. Of those that a mesh axis runs over, the one named last changes fastest.
Arguments:
- inv_diag: float32 [16, 1088, 1088], P('row', None, 'col'), may hold values from -0.1875 to 0.1875
- low_left: float32 [16, 1088, 96], P('row', 'col'), may hold values from -0.1875 to 0.1875
- low_right: float32 [16, 1088, 96], P('row', 'col'), may hold values from -0.625 to 0.625
- deriv_diag: bfloat16 [3, 16, 1088, 1088], P(None, 'row', None, 'col'), may hold values from -0.1875 to 0.1875
- deriv_left: float32 [3, 16, 1088, 96], P(None, 'row', 'col'), may hold values from -0.1875 to 0.1875
- deriv_right: float32 [3, 16, 1088, 96], P(None, 'row', 'col'), may hold values from -0.625 to 0.625
- ranks: int32 [4, 16], P(None, 'row'), may hold values from 88 to 96
- whitened: float32 [17408], P(('row', 'col')), may hold values from -6 to 6
- probes: int32 [8, 17408], P(None, ('row', 'col')), may hold values from -1 to 1, as said below
Outputs:
- solved: float32 [9, 17408], P(None, ('row', 'col'))
- whitened_deriv: float32 [3, 8, 17408], P(None, None, ('row', 'col'))
- fisher: float32 [3, 3], replicated
- score: float32 [3], replicated
The draws below stay inside these ranges and needn't reach their ends.
Inputs may be any that keep to these rules, and one draw needn't show every extreme that they name: `probes`: every entry is -1 or +1. `ranks`: column 0 belongs to no tile.
All inputs are finite; a program needn't handle non-finite values.
Results may differ from the reference program's by a relative error of at most 0.0019.
Values sent between devices are 32-bit elements; how exact they have to be, the bound alone decides.
A program may use at most 64 MiB of HBM per device.

```python
import jax
import jax.numpy as jnp
from jax import lax

B = 1088
RMAX = 96
PROBES = 8
PARAMS = 3
NT = 16
NTOT = 17408


def draw_probes(key, part):
    bits = jax.random.randint(key, (PROBES, NTOT), 0, 2)
    return (2 * bits - 1).astype(jnp.int32)


def place_ends(drawn, key, smallest, high):
    longest = drawn.shape.index(max(drawn.shape))
    spots = []
    for shift in (0, 1):
        where = [jax.random.randint(jax.random.fold_in(key, axis), (), 0, length) for axis, length in enumerate(drawn.shape)]
        where[longest] = (where[longest] + shift) % drawn.shape[longest]
        spots.append(tuple(where))
    return drawn.at[spots[0]].set(smallest).at[spots[1]].set(high)


def block_levels(own_key, extent, cuts, low, top_value):
    def one(axis_at, blocks):
        heights = jax.random.uniform(jax.random.fold_in(jax.random.fold_in(own_key, 6), axis_at), (blocks,), jnp.float32, low / len(cuts), top_value / len(cuts))
        return jnp.repeat(jnp.exp(heights), extent[axis_at] // blocks).reshape((-1,) + (1,) * (len(extent) - axis_at - 1))

    factor_of = one(*cuts[0])
    for cut in cuts[1:]:
        factor_of = factor_of * one(*cut)
    return factor_of


def centred(rng, dims, scale, limit, cuts=(), held_as=jnp.bfloat16):
    array = jax.random.normal(rng, dims, jnp.float32) * scale
    if len(cuts) > 0:
        array = block_levels(rng, dims, cuts, -0.22, 0.18) * array
    return jnp.clip(array, min=-limit, max=limit).astype(held_as)


def setup_inputs(seed: int = 0) -> dict:
    splits = jax.random.split(jax.random.key(seed), 10)
    return {
        "inv_diag": centred(splits[0], (NT, B, B), B ** -0.5, 0.1875, ((0, 16), (2, 2)), jnp.float32),
        "low_left": centred(splits[1], (NT, B, RMAX), B ** -0.5, 0.1875, ((0, 16), (1, 2)), jnp.float32),
        "low_right": centred(splits[2], (NT, B, RMAX), (RMAX - 4) ** -0.5, 0.625, ((0, 16), (1, 2)), jnp.float32),
        "deriv_diag": centred(splits[3], (PARAMS, NT, B, B), B ** -0.5, 0.1875, ((1, 16), (3, 2))),
        "deriv_left": centred(splits[4], (PARAMS, NT, B, RMAX), B ** -0.5, 0.1875, ((1, 16), (2, 2)), jnp.float32),
        "deriv_right": centred(splits[5], (PARAMS, NT, B, RMAX), RMAX ** -0.5, 0.625, ((1, 16), (2, 2)), jnp.float32),
        "ranks": place_ends(jax.random.randint(splits[6], (PARAMS + 1, NT), RMAX - 8, RMAX + 1), jax.random.fold_in(splits[6], 1), RMAX - 8, RMAX).astype(jnp.int32),
        "whitened": centred(splits[7], (NTOT,), 1.0, 6.0, ((0, 32),), jnp.float32),
        "probes": draw_probes(jax.random.fold_in(splits[9], 71), 0),
    }


def reference(inv_diag, low_left, low_right, deriv_diag, deriv_left, deriv_right, ranks, whitened, probes):
    highest = lax.Precision.HIGHEST
    tiles, size, rmax = low_left.shape
    params = deriv_left.shape[0]
    count = probes.shape[0]
    total = tiles * size
    columns = jnp.arange(rmax, dtype=jnp.int32)
    masks = (columns[None, None, :] < ranks[:, :, None]).astype(jnp.float32)
    masked_right = low_right * masks[0][:, None, :]
    deriv_masked = deriv_right * masks[1:][:, :, None, :]
    source = jnp.concatenate([whitened[None, :], probes.astype(jnp.float32)], axis=0)
    source = source.reshape(count + 1, tiles, size).transpose(1, 0, 2)
    empty_factor = jnp.zeros((1, size, rmax), jnp.float32)
    next_left = jnp.concatenate([low_left[1:], empty_factor], 0)
    next_right = jnp.concatenate([masked_right[1:], empty_factor], 0)

    def backward(later, item):
        inverse, left, right, rows = item
        coeff = jnp.dot(later, left, precision=highest)
        rest = rows - jnp.dot(coeff, right.T, precision=highest)
        current = jnp.dot(rest, inverse, precision=highest)
        return current, current

    start = jnp.zeros((count + 1, size), jnp.float32)
    _, solved_tiles = lax.scan(backward, start, (inv_diag, next_left, next_right, source), reverse=True)

    rounded = solved_tiles.astype(jnp.bfloat16)

    def dense_one(index):
        block = lax.dynamic_index_in_dim(deriv_diag, index, 1, keepdims=False)
        rows = lax.dynamic_index_in_dim(rounded, index, 0, keepdims=False)
        return jnp.stack([jnp.dot(rows, block[k].T, preferred_element_type=jnp.float32) for k in range(params)])

    dense = lax.map(dense_one, jnp.arange(tiles, dtype=jnp.int32))
    zero_tile = jnp.zeros((1, count + 1, size), jnp.float32)
    prior = jnp.concatenate([zero_tile, solved_tiles[:-1]], 0)
    lower_coeff = jnp.einsum('tpb,ktbr->ktpr', prior, deriv_masked, precision=highest)
    lower = jnp.einsum('ktpr,ktbr->tkpb', lower_coeff, deriv_left, precision=highest)
    upper_coeff = jnp.einsum('tpb,ktbr->ktpr', solved_tiles, deriv_left, precision=highest)
    upper_here = jnp.einsum('ktpr,ktbr->tkpb', upper_coeff, deriv_masked, precision=highest)
    zero_block = jnp.zeros((1, params, count + 1, size), jnp.float32)
    upper = jnp.concatenate([upper_here[1:], zero_block], 0)
    applied = dense + lower + upper

    drive = applied[:, :, 1:].reshape(tiles, params * count, size)

    def forward(earlier, item):
        inverse, left, right, rows = item
        coeff = jnp.dot(earlier, right, precision=highest)
        rest = rows - jnp.dot(coeff, left.T, precision=highest)
        current = jnp.dot(rest, inverse.T, precision=highest)
        return current, current

    begin = jnp.zeros((params * count, size), jnp.float32)
    _, deriv_tiles = lax.scan(forward, begin, (inv_diag, low_left, masked_right, drive))
    four = deriv_tiles.reshape(tiles, params, count, size)
    solved = solved_tiles.transpose(1, 0, 2).reshape(count + 1, total)
    whitened_deriv = four.transpose(1, 2, 0, 3).reshape(params, count, total)
    trace = jnp.einsum('tkpb,tpb->k', four, source[:, 1:], precision=highest)
    fisher = jnp.einsum('tkpb,tlpb->kl', four, four, precision=highest) / (2.0 * count * total)
    data = jnp.einsum('tkb,tb->k', applied[:, :, 0], solved_tiles[:, 0], precision=highest)
    score = (data - trace / count) / (2.0 * total)
    return solved, whitened_deriv, fisher, score
```

```python
import functools

import jax
import jax.numpy as jnp
from jax import lax
from jax.experimental import pallas as pl
from jax.experimental.pallas import tpu as pltpu
from jax.sharding import PartitionSpec as P

f32, bf16 = jnp.float32, jnp.bfloat16
MESH = pl.DeviceIdType.MESH
NN = (((1,), (0,)), ((), ()))
NT = (((1,), (1,)), ((), ()))


def split(x):
    high = x.astype(bf16)
    return high, (x - high.astype(f32)).astype(bf16)


def dot1(a, b, dims):
    return lax.dot_general(a, b, dims, preferred_element_type=f32)


def dot3(a, b, dims):
    return dot1(a[0], b[0], dims) + (dot1(a[0], b[1], dims) + dot1(a[1], b[0], dims))


def mul(a, b, dims=NN):
    return dot3(split(a), split(b), dims)


def group_size(rows):
    return max(d for d in range(1, rows + 1) if rows % d == 0 and d * d <= rows)


def kernel(
    rows, q_hbm, u_hbm, v_hbm, d_hbm, du_hbm, dv_hbm, ranks_hbm, white_hbm, probes_hbm,
    solved_ref, deriv_ref, fisher_ref, score_ref,
    ranks_ref, white_ref, probes_ref, q, u, own_v, d, du, dv, q_high, q_low, v_all, src_all,
    du_high, du_low, dv_high, dv_low,
    m_part, m_other, m_all, lin_all, off_all, x_own, x_prior, up_part, up_other, up_send, up_recv,
    dense_send, dense_recv, low_part, low_other, s_part, s_other, s_all, o_all,
    w_send, w_recv, tot_all,
    load_sem, pair_send, pair_recv, row_send, row_recv,
    g1_send, g1_recv, l_send, l_recv, g2_send, g2_recv, g3_send, g3_recv, g4_send, g4_recv, tot_send, tot_recv,
):
    i, c = lax.axis_index("row"), lax.axis_index("col")
    p = 1 - c
    half, size = q.shape
    rmax = u.shape[0]
    params = d.shape[0]
    count = s_part.shape[0] // params
    pad = src_all.shape[1]
    group = m_all.shape[0]
    groups = lin_all.shape[0]
    g, l = i // group, i % group

    loads = [
        pltpu.make_async_copy(u_hbm.at[0], u, load_sem.at[0]),
        pltpu.make_async_copy(q_hbm.at[0], q, load_sem.at[1]),
        pltpu.make_async_copy(du_hbm.at[:, 0], du, load_sem.at[2]),
        pltpu.make_async_copy(dv_hbm.at[:, 0], dv, load_sem.at[3]),
        pltpu.make_async_copy(d_hbm.at[:, 0], d, load_sem.at[4]),
    ]
    own_v_load = pltpu.make_async_copy(v_hbm.at[0], own_v, load_sem.at[5])
    small_loads = [
        pltpu.make_async_copy(probes_hbm, probes_ref, load_sem.at[6]),
        pltpu.make_async_copy(white_hbm, white_ref, load_sem.at[7]),
        pltpu.make_async_copy(ranks_hbm, ranks_ref, load_sem.at[8]),
    ]
    own_v_load.start()
    for load in small_loads:
        load.start()
    for load in loads:
        load.start()

    barrier = pltpu.get_barrier_semaphore()

    def greet(k, carry):
        row = lax.rem(i + k, rows)
        for col in range(2):
            @pl.when(jnp.logical_or(k > 0, col != c))
            def _():
                pl.semaphore_signal(barrier, inc=1, device_id=(row, col), device_id_type=MESH)
        return carry

    lax.fori_loop(0, rows, greet, 0)
    pl.semaphore_wait(barrier, 2 * rows - 1)

    def pair(k, src, dst):
        return pltpu.make_async_remote_copy(
            src_ref=src, dst_ref=dst, send_sem=pair_send.at[k], recv_sem=pair_recv.at[k],
            device_id=(i, p), device_id_type=MESH,
        )

    def hop(k, src, dst, distance):
        return pltpu.make_async_remote_copy(
            src_ref=src, dst_ref=dst, send_sem=row_send.at[k], recv_sem=row_recv.at[k],
            device_id=(lax.rem(i + distance + rows, rows), c), device_id_type=MESH,
        )

    own_v_load.wait()
    v_hop = hop(0, own_v, v_all.at[c], -1)

    @pl.when(i > 0)
    def _():
        v_hop.start()

    for load in small_loads:
        load.wait()
    signs = probes_ref[...].astype(f32)
    src_own = jnp.concatenate(
        [signs, white_ref[...].reshape(1, half), jnp.zeros((pad - count - 1, half), f32)], axis=0
    )
    src_all[c] = src_own
    src_pair = pair(0, src_all.at[c], src_all.at[c])
    src_pair.start()

    lane_of = lax.broadcasted_iota(jnp.int32, (1, rmax), 1)
    row_of = lax.broadcasted_iota(jnp.int32, (rmax, 1), 0)
    masks = [(lane_of < ranks_ref[:, k:k + 1]).astype(f32) for k in range(params + 1)]
    loads[0].wait()
    u[...] = u[...] * (row_of < ranks_ref[:, 0:1]).astype(f32)
    u_split = split(u[...])
    loads[1].wait()
    q_high[...], q_low[...] = split(q[...])

    v_pair = pair(1, v_all.at[c], v_all.at[c])

    @pl.when(i < rows - 1)
    def _():
        v_hop.wait_recv()

    @pl.when(i == rows - 1)
    def _():
        v_all[c] = jnp.zeros((rmax, half), f32)

    v_pair.start()
    src_pair.wait_recv()
    v_pair.wait_recv()

    halves = [jnp.concatenate([v_all[s], src_all[s]], axis=0) for s in range(2)]
    both = dot3(split(jnp.concatenate(halves, axis=1)), (q_high[...], q_low[...]), NT)
    wide_t, base = both[:rmax], both[rmax:]
    wide_split = split(wide_t)
    m_part[...] = dot3(split(both), u_split, NT)
    m_pair = pair(2, m_part, m_other)
    m_pair.start()
    m_pair.wait_recv()
    m_own = m_part[...] + m_other[...]
    m_all[l] = m_own

    def spread(block, mine, send, recv, span, device):
        copies = []
        for k in range(1, span):
            copies.append(pltpu.make_async_remote_copy(
                src_ref=block.at[mine], dst_ref=block.at[mine],
                send_sem=send.at[k], recv_sem=recv.at[k],
                device_id=(device(lax.rem(mine + k, span)), c), device_id_type=MESH,
            ))
        for copy in copies:
            copy.start()
        return copies

    in_group = lambda member: g * group + member
    across = lambda other: other * group + l

    g1 = spread(m_all, l, g1_send, g1_recv, group, in_group)
    for load in loads[2:4]:
        load.wait()
    for k in range(params):
        du_high[k], du_low[k] = split(du[k])
        dv_high[k], dv_low[k] = split(dv[k])
    for copy in g1:
        copy.wait_recv()
    m_split = [split(m_all[m, :rmax]) for m in range(group)]
    lift = [m_all[m, rmax:] for m in range(group)]
    lin, off = -m_all[group - 1, :rmax], lift[group - 1]
    for m in reversed(range(group - 1)):
        state = dot3(split(jnp.concatenate([lin, off], axis=0)), m_split[m], NN)
        lin, off = -state[:rmax], lift[m] - state[rmax:]
    lin_all[g] = lin
    off_all[g] = off

    def to_groups(block, send, recv):
        return [
            pltpu.make_async_remote_copy(
                src_ref=block.at[g], dst_ref=block.at[g],
                send_sem=send.at[m], recv_sem=recv.at[g],
                device_id=(across(m), c), device_id_type=MESH,
            )
            for m in range(groups)
        ]

    def from_group(block, recv, m):
        return pltpu.make_async_remote_copy(
            src_ref=block.at[m], dst_ref=block.at[m],
            send_sem=recv.at[m], recv_sem=recv.at[m],
            device_id=(across(m), c), device_id_type=MESH,
        )

    def when_each(test, act, items):
        for m, item in enumerate(items):
            @pl.when(test(m))
            def _():
                act(item)

    everyone = list(range(groups))
    inner = jnp.logical_and(g > 0, g < groups - 1)
    lin_copies = to_groups(lin_all, l_send, l_recv)
    off_copies = to_groups(off_all, g2_send, g2_recv)
    when_each(lambda m: m < g, lambda copy: copy.start(), off_copies)
    when_each(lambda m: jnp.logical_and(inner, m != g), lambda copy: copy.start(), lin_copies)
    when_each(lambda m: m > g, lambda m: from_group(off_all, g2_recv, m).wait_recv(), everyone)
    for m in range(1, groups - 1):
        @pl.when(m != g)
        def _():
            from_group(lin_all, l_recv, m).wait_recv()
    t_split = [split(lin_all[m]) for m in range(groups)]
    a = jnp.zeros((pad, rmax), f32)
    for m in reversed(range(1, groups)):
        new = off_all[m]
        if m < groups - 1:
            new = new + dot3(split(a), t_split[m], NN)
        a = jnp.where(m > g, new, a)
    for m in reversed(range(1, group)):
        a = jnp.where(m > l, lift[m] - dot3(split(a), m_split[m], NN), a)

    x = base - dot3(split(a), wide_split, NN)
    x_own[...] = x
    x_hop = hop(1, x_own, x_prior, 1)

    @pl.when(i < rows - 1)
    def _():
        x_hop.start()

    x_split = split(x)
    du_split = [(du_high[k], du_low[k]) for k in range(params)]
    dv_split = [(dv_high[k], dv_low[k]) for k in range(params)]
    for k in range(params):
        up_part[k] = dot3(x_split, du_split[k], NT)
    up_pair = pair(3, up_part, up_other)
    up_pair.start()
    solved_ref[0:1] = x[count:count + 1]
    solved_ref[1:] = x[:count]
    rounded = x_split[0]
    loads[4].wait()

    def pack(ref, k, block):
        ref[k * count:(k + 1) * count] = block[:count]
        ref[params * count + k:params * count + k + 1] = block[count:count + 1]

    def halves_of(block):
        low, high = block[:, :half], block[:, half:]
        return jnp.where(c == 0, low, high), jnp.where(c == 0, high, low)

    dense = [halves_of(dot1(rounded, d[k], NN)) for k in range(params)]
    for k in range(params):
        pack(dense_send, k, dense[k][1])
    dense_pair = pair(4, dense_send, dense_recv)
    dense_pair.start()
    up_pair.wait_recv()
    for k in range(params):
        coeff = (up_part[k] + up_other[k]) * masks[k + 1]
        pack(up_send, k, dot3(split(coeff), dv_split[k], NN))
    up_hop = hop(2, up_send, up_recv, -1)

    @pl.when(i > 0)
    def _():
        up_hop.start()

    @pl.when(i > 0)
    def _():
        x_hop.wait_recv()

    @pl.when(i == 0)
    def _():
        x_prior[...] = jnp.zeros((pad, half), f32)

    prior_split = split(x_prior[...])
    for k in range(params):
        low_part[k] = dot3(prior_split, dv_split[k], NT)
    low_pair = pair(5, low_part, low_other)
    low_pair.start()
    low_pair.wait_recv()
    lower = []
    for k in range(params):
        coeff = (low_part[k] + low_other[k]) * masks[k + 1]
        lower.append(dense[k][0] + dot3(split(coeff), du_split[k], NN))
    dense_pair.wait_recv()

    @pl.when(i < rows - 1)
    def _():
        up_hop.wait_recv()

    @pl.when(i == rows - 1)
    def _():
        up_recv[...] = jnp.zeros(up_recv.shape, f32)

    other = dense_recv[...] + up_recv[...]
    drive = jnp.concatenate([part[:count] for part in lower], axis=0) + other[:params * count]
    observed = [
        lower[k][count:count + 1] + other[params * count + k:params * count + k + 1]
        for k in range(params)
    ]
    s_part[...] = dot3(split(drive), wide_split, NT)
    s_pair = pair(6, s_part, s_other)
    s_pair.start()
    s_pair.wait_recv()
    s_all[l] = s_part[...] + s_other[...]
    g3 = spread(s_all, l, g3_send, g3_recv, group, in_group)
    for copy in g3:
        copy.wait_recv()
    total = s_all[0]
    for m in range(1, group):
        total = s_all[m] - dot3(split(total), m_split[m], NT)
    o_all[g] = total
    o_copies = to_groups(o_all, g4_send, g4_recv)
    when_each(lambda m: m > g, lambda copy: copy.start(), o_copies)
    when_each(lambda m: m < g, lambda m: from_group(o_all, g4_recv, m).wait_recv(), everyone)
    b = jnp.zeros((params * count, rmax), f32)
    for m in range(groups - 1):
        new = o_all[m]
        if m > 0:
            new = new + dot3(split(b), t_split[m], NT)
        b = jnp.where(m < g, new, b)
    for m in range(group - 1):
        b = jnp.where(m < l, s_all[m] - dot3(split(b), m_split[m], NT), b)

    rest = split(drive - dot3(split(b), u_split, NN))
    w, w_send[...] = halves_of(dot3(rest, (q_high[...], q_low[...]), NN))
    w_pair = pair(7, w_send, w_recv)
    w_pair.start()
    w_pair.wait_recv()
    w = w + w_recv[...]
    parts = [w[k * count:(k + 1) * count] for k in range(params)]
    for k in range(params):
        deriv_ref[k] = parts[k]

    lanes = tot_all.shape[2]
    lane = lax.broadcasted_iota(jnp.int32, (1, lanes), 1)
    packed = jnp.zeros((1, lanes), f32)

    def put(packed, at, value):
        summed = jnp.sum(jnp.sum(value, axis=0, keepdims=True), axis=1, keepdims=True)
        return jnp.where(lane == at, summed, packed)

    for k in range(params):
        for m in range(k, params):
            product = parts[k] * parts[m]
            packed = put(packed, k * params + m, product)
        packed = put(packed, params * params + k, parts[k] * signs)
        data = observed[k] * x[count:count + 1]
        packed = put(packed, params * params + params + k, data)
    me = 2 * i + c
    devices = 2 * rows
    tot_all[me] = packed

    def tot_copy(k):
        other = lax.rem(me + k, devices)
        return pltpu.make_async_remote_copy(
            src_ref=tot_all.at[me], dst_ref=tot_all.at[me],
            send_sem=tot_send.at[k], recv_sem=tot_recv.at[k],
            device_id=(other // 2, lax.rem(other, 2)), device_id_type=MESH,
        )

    def tot_start(k, carry):
        tot_copy(k).start()
        return carry

    def tot_wait(k, carry):
        tot_copy(k).wait()
        return carry

    lax.fori_loop(1, devices, tot_start, 0)

    for copy in (src_pair, v_pair, m_pair, up_pair, dense_pair, low_pair, s_pair, w_pair):
        copy.wait_send()
    for copy in g1 + g3:
        copy.wait_send()
    when_each(lambda m: m < g, lambda copy: copy.wait_send(), off_copies)
    when_each(lambda m: jnp.logical_and(inner, m != g), lambda copy: copy.wait_send(), lin_copies)
    when_each(lambda m: m > g, lambda copy: copy.wait_send(), o_copies)

    @pl.when(i > 0)
    def _():
        v_hop.wait_send()
        up_hop.wait_send()

    @pl.when(i < rows - 1)
    def _():
        x_hop.wait_send()

    lax.fori_loop(1, devices, tot_wait, 0)
    sums = jnp.sum(tot_all[...], axis=0)
    locations = rows * size
    for k in range(params):
        for m in range(params):
            at = min(k, m) * params + max(k, m)
            fisher_ref[k:k + 1, m:m + 1] = sums[:, at:at + 1] / (2.0 * count * locations)
    at = params * params
    trace, data = sums[:, at:at + params], sums[:, at + params:at + 2 * params]
    score_ref[...] = (data - trace / count) / (2.0 * locations)


def store(*refs):
    sem = refs[-1]
    copies = [pltpu.make_async_copy(refs[k], refs[k + 4], sem.at[k]) for k in range(4)]
    for copy in copies:
        copy.start()
    for copy in copies:
        copy.wait()


def body(
    inv_diag, low_left, low_right, deriv_diag, deriv_left, deriv_right, ranks, whitened, probes
):
    rows = lax.axis_size("row")
    _, size, half = inv_diag.shape
    rmax = low_left.shape[2]
    params = deriv_left.shape[0]
    count = probes.shape[0]
    pad = -(-(count + 1) // 8) * 8
    group = group_size(rows)
    groups = rows // group
    devices = 2 * rows
    lanes = -(-(params * params + 2 * params) // 128) * 128
    vm, dma = pltpu.VMEM, pltpu.SemaphoreType.DMA
    high = rmax + pad
    packed = -(-params * (count + 1) // 8) * 8
    outs = pl.pallas_call(
        functools.partial(kernel, rows),
        out_shape=(
            vm((count + 1, half), f32), vm((params, count, half), f32),
            vm((params, params), f32), vm((1, params), f32),
        ),
        in_specs=[pl.BlockSpec(memory_space=pltpu.HBM)] * 9,
        out_specs=[pl.BlockSpec(memory_space=pltpu.VMEM)] * 4,
        scratch_shapes=[
            vm((1, params + 1), jnp.int32), vm((half,), f32), vm((count, half), jnp.int32),
            vm((half, size), f32), vm((rmax, half), f32), vm((rmax, half), f32),
            vm((params, half, size), bf16), vm((params, rmax, half), f32),
            vm((params, rmax, half), f32), vm((half, size), bf16), vm((half, size), bf16),
            vm((2, rmax, half), f32), vm((2, pad, half), f32),
            vm((params, rmax, half), bf16), vm((params, rmax, half), bf16),
            vm((params, rmax, half), bf16), vm((params, rmax, half), bf16),
            vm((high, rmax), f32), vm((high, rmax), f32), vm((group, high, rmax), f32),
            vm((groups, rmax, rmax), f32), vm((groups, pad, rmax), f32),
            vm((pad, half), f32), vm((pad, half), f32),
            vm((params, pad, rmax), f32), vm((params, pad, rmax), f32),
            vm((packed, half), f32), vm((packed, half), f32),
            vm((packed, half), f32), vm((packed, half), f32),
            vm((params, pad, rmax), f32), vm((params, pad, rmax), f32),
            vm((params * count, rmax), f32), vm((params * count, rmax), f32),
            vm((group, params * count, rmax), f32), vm((groups, params * count, rmax), f32),
            vm((params * count, half), f32), vm((params * count, half), f32),
            vm((devices, 1, lanes), f32),
            dma((9,)), dma((8,)), dma((8,)), dma((3,)), dma((3,)),
            dma((group,)), dma((group,)), dma((groups,)), dma((groups,)), dma((groups,)), dma((groups,)),
            dma((group,)), dma((group,)), dma((groups,)), dma((groups,)),
            dma((devices,)), dma((devices,)),
        ],
        compiler_params=pltpu.CompilerParams(
            collective_id=0, has_side_effects=True, vmem_limit_bytes=60 * 1024 * 1024
        ),
    )(
        *[jnp.swapaxes(x, -1, -2) for x in (
            inv_diag, low_left, low_right, deriv_diag, deriv_left, deriv_right, ranks
        )],
        whitened, probes,
    )
    outs = pl.pallas_call(
        store,
        out_shape=tuple(jax.ShapeDtypeStruct(x.shape, x.dtype) for x in outs),
        in_specs=[pl.BlockSpec(memory_space=pltpu.VMEM)] * 4,
        out_specs=[pl.BlockSpec(memory_space=pltpu.HBM)] * 4,
        scratch_shapes=[dma((4,))],
    )(*[pltpu.with_memory_space_constraint(x, pltpu.VMEM) for x in outs])
    return outs[0], outs[1], outs[2], outs[3][0]


def solution(mesh):
    return jax.shard_map(
        body,
        mesh=mesh,
        in_specs=(
            P("row", None, "col"),
            P("row", "col", None),
            P("row", "col", None),
            P(None, "row", None, "col"),
            P(None, "row", "col", None),
            P(None, "row", "col", None),
            P(None, "row"),
            P(("row", "col")),
            P(None, ("row", "col")),
        ),
        out_specs=(P(None, ("row", "col")), P(None, None, ("row", "col")), P(), P()),
        check_vma=False,
    )
```

```python
import functools

import jax
import jax.numpy as jnp
from jax import lax
from jax.experimental import pallas as pl
from jax.experimental.pallas import tpu as pltpu
from jax.sharding import PartitionSpec as P

f32, bf16 = jnp.float32, jnp.bfloat16
MESH = pl.DeviceIdType.MESH
NN = (((1,), (0,)), ((), ()))
NT = (((1,), (1,)), ((), ()))


def split(x):
    high = x.astype(bf16)
    return high, (x - high.astype(f32)).astype(bf16)


def dot1(a, b, dims):
    return lax.dot_general(a, b, dims, preferred_element_type=f32)


def dot3(a, b, dims):
    return dot1(a[0], b[0], dims) + (dot1(a[0], b[1], dims) + dot1(a[1], b[0], dims))


def mul(a, b, dims=NN):
    return dot3(split(a), split(b), dims)


def group_size(rows):
    return max(d for d in range(1, rows + 1) if rows % d == 0 and d * d <= rows)


def kernel(
    rows, q_hbm, u_hbm, v_hbm, d_hbm, du_hbm, dv_hbm, ranks_hbm, white_hbm, probes_hbm,
    solved_ref, deriv_ref, fisher_ref, score_ref,
    ranks_ref, white_ref, probes_ref, q, u, own_v, d, du, dv, q_high, q_low, v_all, src_all,
    du_high, du_low, dv_high, dv_low, p_send, p_recv, p_high, p_low, wd_part, wd_other,
    m_part, m_other, m_all, lin_all, off_all, x_own, x_prior, up_send, up_recv,
    dense_own, dense_send, dense_recv, low_part, low_other, s_all, o_all,
    w_send, w_recv, tot_all,
    load_sem, pair_send, pair_recv, row_send, row_recv,
    g1_send, g1_recv, l_send, l_recv, g2_send, g2_recv, g3_send, g3_recv, g4_send, g4_recv, tot_send, tot_recv,
):
    i, c = lax.axis_index("row"), lax.axis_index("col")
    p = 1 - c
    half, size = q.shape
    rmax = u.shape[0]
    params = d.shape[0]
    count = probes_ref.shape[0]
    pad = src_all.shape[1]
    group = m_all.shape[0]
    groups = lin_all.shape[0]
    g, l = i // group, i % group

    loads = [
        pltpu.make_async_copy(u_hbm.at[0], u, load_sem.at[0]),
        pltpu.make_async_copy(q_hbm.at[0], q, load_sem.at[1]),
        pltpu.make_async_copy(du_hbm.at[:, 0], du, load_sem.at[2]),
        pltpu.make_async_copy(dv_hbm.at[:, 0], dv, load_sem.at[3]),
        pltpu.make_async_copy(d_hbm.at[:, 0], d, load_sem.at[4]),
    ]
    own_v_load = pltpu.make_async_copy(v_hbm.at[0], own_v, load_sem.at[5])
    small_loads = [
        pltpu.make_async_copy(probes_hbm, probes_ref, load_sem.at[6]),
        pltpu.make_async_copy(white_hbm, white_ref, load_sem.at[7]),
        pltpu.make_async_copy(ranks_hbm, ranks_ref, load_sem.at[8]),
    ]
    own_v_load.start()
    for load in small_loads:
        load.start()
    for load in loads:
        load.start()

    barrier = pltpu.get_barrier_semaphore()

    def greet(k, carry):
        row = lax.rem(i + k, rows)
        for col in range(2):
            @pl.when(jnp.logical_or(k > 0, col != c))
            def _():
                pl.semaphore_signal(barrier, inc=1, device_id=(row, col), device_id_type=MESH)
        return carry

    lax.fori_loop(0, rows, greet, 0)
    pl.semaphore_wait(barrier, 2 * rows - 1)

    def pair(k, src, dst):
        return pltpu.make_async_remote_copy(
            src_ref=src, dst_ref=dst, send_sem=pair_send.at[k], recv_sem=pair_recv.at[k],
            device_id=(i, p), device_id_type=MESH,
        )

    def hop(k, src, dst, distance):
        return pltpu.make_async_remote_copy(
            src_ref=src, dst_ref=dst, send_sem=row_send.at[k], recv_sem=row_recv.at[k],
            device_id=(lax.rem(i + distance + rows, rows), c), device_id_type=MESH,
        )

    def halves_of(block):
        low, high = block[:, :half], block[:, half:]
        return jnp.where(c == 0, low, high), jnp.where(c == 0, high, low)

    own_v_load.wait()
    v_hop = hop(0, own_v, v_all.at[c], -1)

    @pl.when(i > 0)
    def _():
        v_hop.start()

    for load in small_loads:
        load.wait()
    signs = probes_ref[...].astype(f32)
    src_own = jnp.concatenate(
        [signs, white_ref[...].reshape(1, half), jnp.zeros((pad - count - 1, half), f32)], axis=0
    )
    src_all[c] = src_own
    src_pair = pair(0, src_all.at[c], src_all.at[c])
    src_pair.start()

    row_of = lax.broadcasted_iota(jnp.int32, (rmax, 1), 0)
    loads[0].wait()
    u_split = split(u[...] * (row_of < ranks_ref[:, 0:1]).astype(f32))
    loads[1].wait()
    q_high[...], q_low[...] = split(q[...])
    p_own, p_send[...] = halves_of(dot3(u_split, (q_high[...], q_low[...]), NN))
    p_pair = pair(1, p_send, p_recv)
    p_pair.start()
    for load in loads[2:4]:
        load.wait()
    for k in range(params):
        du_high[k], du_low[k] = split(du[k] * (row_of < ranks_ref[:, k + 1:k + 2]).astype(f32))
        dv_high[k], dv_low[k] = split(dv[k])
    p_pair.wait_recv()
    p_high[...], p_low[...] = split(p_own + p_recv[...])
    src_pair.wait_recv()

    v_pair = pair(2, v_all.at[c], v_all.at[c])

    @pl.when(i < rows - 1)
    def _():
        v_hop.wait_recv()

    @pl.when(i == rows - 1)
    def _():
        v_all[c] = jnp.zeros((rmax, half), f32)

    v_pair.start()
    p_split = (p_high[...], p_low[...])
    m_part[...] = dot3(split(jnp.concatenate([v_all[c], src_own], axis=0)), p_split, NT)
    m_pair = pair(3, m_part, m_other)
    m_pair.start()
    m_pair.wait_recv()
    m_all[l] = m_part[...] + m_other[...]

    def spread(block, mine, send, recv, span, device):
        copies = []
        for k in range(1, span):
            copies.append(pltpu.make_async_remote_copy(
                src_ref=block.at[mine], dst_ref=block.at[mine],
                send_sem=send.at[k], recv_sem=recv.at[k],
                device_id=(device(lax.rem(mine + k, span)), c), device_id_type=MESH,
            ))
        for copy in copies:
            copy.start()
        return copies

    in_group = lambda member: g * group + member
    across = lambda other: other * group + l

    g1 = spread(m_all, l, g1_send, g1_recv, group, in_group)

    v_pair.wait_recv()
    halves = [jnp.concatenate([v_all[s], src_all[s]], axis=0) for s in range(2)]
    both = dot3(split(jnp.concatenate(halves, axis=1)), (q_high[...], q_low[...]), NT)
    base = both[rmax:]
    both_split = split(both)
    wide_split = tuple(part[:rmax] for part in both_split)
    du_split = [(du_high[k], du_low[k]) for k in range(params)]
    dv_split = [(dv_high[k], dv_low[k]) for k in range(params)]
    for k in range(params):
        wd_part[k] = dot3(both_split, du_split[k], NT)
    wd_pair = pair(4, wd_part, wd_other)
    wd_pair.start()

    for copy in g1:
        copy.wait_recv()
    m_split = [split(m_all[m, :rmax]) for m in range(group)]
    lift = [m_all[m, rmax:] for m in range(group)]
    lin, off = -m_all[group - 1, :rmax], lift[group - 1]
    own_lin, own_off = lin, off
    lin_split = {group - 1: split(lin)}
    for m in reversed(range(group - 1)):
        own_lin, own_off = jnp.where(l <= m, lin, own_lin), jnp.where(l <= m, off, own_off)
        off_split = split(off)
        state = dot3(
            tuple(jnp.concatenate(part, axis=0) for part in zip(lin_split[m + 1], off_split)), m_split[m], NN
        )
        lin, off = -state[:rmax], lift[m] - state[rmax:]
        if m > 0:
            lin_split[m] = split(lin)
    lin_all[g] = lin
    off_all[g] = off

    def to_groups(block, send, recv):
        return [
            pltpu.make_async_remote_copy(
                src_ref=block.at[g], dst_ref=block.at[g],
                send_sem=send.at[m], recv_sem=recv.at[g],
                device_id=(across(m), c), device_id_type=MESH,
            )
            for m in range(groups)
        ]

    def from_group(block, recv, m):
        return pltpu.make_async_remote_copy(
            src_ref=block.at[m], dst_ref=block.at[m],
            send_sem=recv.at[m], recv_sem=recv.at[m],
            device_id=(across(m), c), device_id_type=MESH,
        )

    def when_each(test, act, items):
        for m, item in enumerate(items):
            @pl.when(test(m))
            def _():
                act(item)

    everyone = list(range(groups))
    inner = jnp.logical_and(g > 0, g < groups - 1)
    lin_copies = to_groups(lin_all, l_send, l_recv)
    off_copies = to_groups(off_all, g2_send, g2_recv)
    when_each(lambda m: m < g, lambda copy: copy.start(), off_copies)
    when_each(lambda m: jnp.logical_and(inner, m != g), lambda copy: copy.start(), lin_copies)

    own_lin_split = split(own_lin)
    lead = -m_all[0, :rmax]
    own_lead = lead
    for m in range(1, group - 1):
        lead = -dot3(m_split[m], split(lead), NN)
        own_lead = jnp.where(l > m, lead, own_lead)
    lead_split = split(own_lead)
    wd_pair.wait_recv()
    wd_split, ub, dvw_split = [], [], []
    for k in range(params):
        wd = wd_part[k] + wd_other[k]
        wd_split.append(split(wd[:rmax]))
        ub.append(wd[rmax:])
        dvw_split.append(split(dot3(wd_split[k], dv_split[k], NN)))

    when_each(lambda m: m > g, lambda m: from_group(off_all, g2_recv, m).wait_recv(), everyone)
    for m in range(1, groups - 1):
        @pl.when(m != g)
        def _():
            from_group(lin_all, l_recv, m).wait_recv()
    t_split = [split(lin_all[m]) for m in range(groups)]
    a = jnp.zeros((pad, rmax), f32)
    for m in reversed(range(1, groups)):
        new = off_all[m]
        if m < groups - 1:
            new = new + dot3(split(a), t_split[m], NN)
        a = jnp.where(m > g, new, a)
    a = jnp.where(l < group - 1, own_off + dot3(split(a), own_lin_split, NN), a)

    a_split = split(a)
    x = base - dot3(a_split, wide_split, NN)
    x_own[...] = x
    x_hop = hop(1, x_own, x_prior, 1)

    @pl.when(i < rows - 1)
    def _():
        x_hop.start()

    def pack(ref, k, block):
        ref[k * count:(k + 1) * count] = block[:count]
        ref[params * count + k:params * count + k + 1] = block[count:count + 1]

    for k in range(params):
        coeff = ub[k] - dot3(a_split, wd_split[k], NN)
        pack(up_send, k, dot3(split(coeff), dv_split[k], NN))
    up_hop = hop(2, up_send, up_recv, -1)

    @pl.when(i > 0)
    def _():
        up_hop.start()

    solved_ref[0:1] = x[count:count + 1]
    solved_ref[1:] = x[:count]
    rounded = x.astype(bf16)
    loads[4].wait()
    for k in range(params):
        mine, theirs = halves_of(dot1(rounded, d[k], NN))
        pack(dense_own, k, mine)
        pack(dense_send, k, theirs)
    dense_pair = pair(5, dense_send, dense_recv)
    dense_pair.start()

    @pl.when(i > 0)
    def _():
        x_hop.wait_recv()

    @pl.when(i == 0)
    def _():
        x_prior[...] = jnp.zeros((pad, half), f32)

    prior_split = split(x_prior[...])
    for k in range(params):
        low_part[k] = dot3(prior_split, dv_split[k], NT)
    low_pair = pair(6, low_part, low_other)
    low_pair.start()
    s_low = jnp.concatenate([dot3(prior_split, dvw_split[k], NT)[:count] for k in range(params)], axis=0)
    dense_pair.wait_recv()

    @pl.when(i < rows - 1)
    def _():
        up_hop.wait_recv()

    @pl.when(i == rows - 1)
    def _():
        up_recv[...] = jnp.zeros(up_recv.shape, f32)

    applied = dense_own[...] + dense_recv[...] + up_recv[...]
    s_all[2 * l + c] = dot3(split(applied[:params * count]), wide_split, NT) + s_low
    g3 = []
    for k in range(group):
        for other in range(2):
            if k > 0 or other > 0:
                g3.append(pltpu.make_async_remote_copy(
                    src_ref=s_all.at[2 * l + c], dst_ref=s_all.at[2 * l + c],
                    send_sem=g3_send.at[2 * k + other], recv_sem=g3_recv.at[2 * k + other],
                    device_id=(in_group(lax.rem(l + k, group)), (c, p)[other]), device_id_type=MESH,
                ))
    for copy in g3:
        copy.start()

    low_pair.wait_recv()
    lower = [dot3(split(low_part[k] + low_other[k]), du_split[k], NN) for k in range(params)]
    drive = applied[:params * count] + jnp.concatenate([block[:count] for block in lower], axis=0)
    observed = [
        applied[params * count + k:params * count + k + 1] + lower[k][count:count + 1] for k in range(params)
    ]
    w, w_send[...] = halves_of(dot3(split(drive), (q_high[...], q_low[...]), NN))
    w_pair = pair(7, w_send, w_recv)
    w_pair.start()

    for copy in g3:
        copy.wait_recv()
    s_sum = [s_all[2 * m] + s_all[2 * m + 1] for m in range(group)]
    s_split = [split(s_sum[m]) for m in range(group - 1)]
    total = s_sum[group - 1]
    for m in range(group - 1):
        total = total + dot3(s_split[m], lin_split[m + 1], NT)
    o_all[g] = total
    o_copies = to_groups(o_all, g4_send, g4_recv)
    when_each(lambda m: m > g, lambda copy: copy.start(), o_copies)
    b = jnp.where(l > 0, s_sum[0], 0.0)
    for m in range(1, group - 1):
        b = jnp.where(m < l, s_sum[m] - dot3(split(b), m_split[m], NT), b)
    w_pair.wait_recv()
    w = w + w_recv[...] - dot3(split(b), p_split, NN)
    when_each(lambda m: m < g, lambda m: from_group(o_all, g4_recv, m).wait_recv(), everyone)
    b = jnp.zeros((params * count, rmax), f32)
    for m in range(groups - 1):
        new = o_all[m]
        if m > 0:
            new = new + dot3(split(b), t_split[m], NT)
        b = jnp.where(m < g, new, b)
    b = jnp.where(l > 0, dot3(split(b), lead_split, NT), b)

    w = w - dot3(split(b), p_split, NN)
    parts = [w[k * count:(k + 1) * count] for k in range(params)]
    for k in range(params):
        deriv_ref[k] = parts[k]

    lanes = tot_all.shape[2]
    lane = lax.broadcasted_iota(jnp.int32, (1, lanes), 1)
    packed = jnp.zeros((1, lanes), f32)

    def put(packed, at, value):
        summed = jnp.sum(jnp.sum(value, axis=0, keepdims=True), axis=1, keepdims=True)
        return jnp.where(lane == at, summed, packed)

    for k in range(params):
        for m in range(k, params):
            product = parts[k] * parts[m]
            packed = put(packed, k * params + m, product)
        packed = put(packed, params * params + k, parts[k] * signs)
        data = observed[k] * x[count:count + 1]
        packed = put(packed, params * params + params + k, data)
    me = 2 * i + c
    devices = 2 * rows
    tot_all[me] = packed

    def tot_copy(k):
        other = lax.rem(me + k, devices)
        return pltpu.make_async_remote_copy(
            src_ref=tot_all.at[me], dst_ref=tot_all.at[me],
            send_sem=tot_send.at[k], recv_sem=tot_recv.at[k],
            device_id=(other // 2, lax.rem(other, 2)), device_id_type=MESH,
        )

    def tot_start(k, carry):
        tot_copy(k).start()
        return carry

    def tot_wait(k, carry):
        tot_copy(k).wait()
        return carry

    lax.fori_loop(1, devices, tot_start, 0)

    for copy in (src_pair, p_pair, v_pair, m_pair, wd_pair, dense_pair, low_pair, w_pair):
        copy.wait_send()
    for copy in g1 + g3:
        copy.wait_send()
    when_each(lambda m: m < g, lambda copy: copy.wait_send(), off_copies)
    when_each(lambda m: jnp.logical_and(inner, m != g), lambda copy: copy.wait_send(), lin_copies)
    when_each(lambda m: m > g, lambda copy: copy.wait_send(), o_copies)

    @pl.when(i > 0)
    def _():
        v_hop.wait_send()
        up_hop.wait_send()

    @pl.when(i < rows - 1)
    def _():
        x_hop.wait_send()

    lax.fori_loop(1, devices, tot_wait, 0)
    sums = jnp.sum(tot_all[...], axis=0)
    locations = rows * size
    for k in range(params):
        for m in range(params):
            at = min(k, m) * params + max(k, m)
            fisher_ref[k:k + 1, m:m + 1] = sums[:, at:at + 1] / (2.0 * count * locations)
    at = params * params
    trace, data = sums[:, at:at + params], sums[:, at + params:at + 2 * params]
    score_ref[...] = (data - trace / count) / (2.0 * locations)


def store(*refs):
    sem = refs[-1]
    copies = [pltpu.make_async_copy(refs[k], refs[k + 4], sem.at[k]) for k in range(4)]
    for copy in copies:
        copy.start()
    for copy in copies:
        copy.wait()


def body(
    inv_diag, low_left, low_right, deriv_diag, deriv_left, deriv_right, ranks, whitened, probes
):
    rows = lax.axis_size("row")
    _, size, half = inv_diag.shape
    rmax = low_left.shape[2]
    params = deriv_left.shape[0]
    count = probes.shape[0]
    pad = -(-(count + 1) // 8) * 8
    group = group_size(rows)
    groups = rows // group
    devices = 2 * rows
    lanes = -(-(params * params + 2 * params) // 128) * 128
    vm, dma = pltpu.VMEM, pltpu.SemaphoreType.DMA
    high = rmax + pad
    packed = -(-params * (count + 1) // 8) * 8
    outs = pl.pallas_call(
        functools.partial(kernel, rows),
        out_shape=(
            vm((count + 1, half), f32), vm((params, count, half), f32),
            vm((params, params), f32), vm((1, params), f32),
        ),
        in_specs=[pl.BlockSpec(memory_space=pltpu.HBM)] * 9,
        out_specs=[pl.BlockSpec(memory_space=pltpu.VMEM)] * 4,
        scratch_shapes=[
            vm((1, params + 1), jnp.int32), vm((half,), f32), vm((count, half), jnp.int32),
            vm((half, size), f32), vm((rmax, half), f32), vm((rmax, half), f32),
            vm((params, half, size), bf16), vm((params, rmax, half), f32),
            vm((params, rmax, half), f32), vm((half, size), bf16), vm((half, size), bf16),
            vm((2, rmax, half), f32), vm((2, pad, half), f32),
            vm((params, rmax, half), bf16), vm((params, rmax, half), bf16),
            vm((params, rmax, half), bf16), vm((params, rmax, half), bf16),
            vm((rmax, half), f32), vm((rmax, half), f32), vm((rmax, half), bf16), vm((rmax, half), bf16),
            vm((params, high, rmax), f32), vm((params, high, rmax), f32),
            vm((high, rmax), f32), vm((high, rmax), f32), vm((group, high, rmax), f32),
            vm((groups, rmax, rmax), f32), vm((groups, pad, rmax), f32),
            vm((pad, half), f32), vm((pad, half), f32),
            vm((packed, half), f32), vm((packed, half), f32),
            vm((packed, half), f32), vm((packed, half), f32), vm((packed, half), f32),
            vm((params, pad, rmax), f32), vm((params, pad, rmax), f32),
            vm((2 * group, params * count, rmax), f32), vm((groups, params * count, rmax), f32),
            vm((params * count, half), f32), vm((params * count, half), f32),
            vm((devices, 1, lanes), f32),
            dma((9,)), dma((8,)), dma((8,)), dma((3,)), dma((3,)),
            dma((group,)), dma((group,)), dma((groups,)), dma((groups,)), dma((groups,)), dma((groups,)),
            dma((2 * group,)), dma((2 * group,)), dma((groups,)), dma((groups,)),
            dma((devices,)), dma((devices,)),
        ],
        compiler_params=pltpu.CompilerParams(
            collective_id=0, has_side_effects=True, vmem_limit_bytes=60 * 1024 * 1024
        ),
    )(
        *[jnp.swapaxes(x, -1, -2) for x in (
            inv_diag, low_left, low_right, deriv_diag, deriv_left, deriv_right, ranks
        )],
        whitened, probes,
    )
    outs = pl.pallas_call(
        store,
        out_shape=tuple(jax.ShapeDtypeStruct(x.shape, x.dtype) for x in outs),
        in_specs=[pl.BlockSpec(memory_space=pltpu.VMEM)] * 4,
        out_specs=[pl.BlockSpec(memory_space=pltpu.HBM)] * 4,
        scratch_shapes=[dma((4,))],
    )(*[pltpu.with_memory_space_constraint(x, pltpu.VMEM) for x in outs])
    return outs[0], outs[1], outs[2], outs[3][0]


def solution(mesh):
    return jax.shard_map(
        body,
        mesh=mesh,
        in_specs=(
            P("row", None, "col"),
            P("row", "col", None),
            P("row", "col", None),
            P(None, "row", None, "col"),
            P(None, "row", "col", None),
            P(None, "row", "col", None),
            P(None, "row"),
            P(("row", "col")),
            P(None, ("row", "col")),
        ),
        out_specs=(P(None, ("row", "col")), P(None, None, ("row", "col")), P(), P()),
        check_vma=False,
    )
```

```python
import functools

import jax
import jax.numpy as jnp
from jax import lax
from jax.experimental import pallas as pl
from jax.experimental.pallas import tpu as pltpu
from jax.sharding import PartitionSpec as P

f32, bf16 = jnp.float32, jnp.bfloat16
MESH = pl.DeviceIdType.MESH
NN = (((1,), (0,)), ((), ()))
NT = (((1,), (1,)), ((), ()))


def split(x):
    high = x.astype(bf16)
    return high, (x - high.astype(f32)).astype(bf16)


def dot1(a, b, dims):
    return lax.dot_general(a, b, dims, preferred_element_type=f32)


def dot3(a, b, dims):
    return dot1(a[0], b[0], dims) + (dot1(a[0], b[1], dims) + dot1(a[1], b[0], dims))


def mul(a, b, dims=NN):
    return dot3(split(a), split(b), dims)


def group_size(rows):
    return max(d for d in range(1, rows + 1) if rows % d == 0 and d * d <= rows)


def kernel(
    rows, q_hbm, u_hbm, v_hbm, d_hbm, du_hbm, dv_hbm, ranks_hbm, white_hbm, probes_hbm,
    solved_ref, deriv_ref, fisher_ref, score_ref,
    ranks_ref, white_ref, probes_ref, q, u, own_v, d, du, dv, q_high, q_low, v_all, src_all,
    du_high, du_low, dv_high, dv_low, p_send, p_recv, p_high, p_low, wd_part, wd_other,
    m_part, m_other, m_all, lin_all, lin_ahead, off_all, x_own, x_prior, up_send, up_recv,
    dense_own, dense_send, dense_recv, low_part, low_other, s_all, o_all,
    w_send, w_recv, tot_all,
    load_sem, pair_send, pair_recv, row_send, row_recv,
    g1_send, g1_recv, l_send, l_recv, g2_send, g2_recv, g3_send, g3_recv, g4_send, g4_recv, tot_send, tot_recv,
):
    i, c = lax.axis_index("row"), lax.axis_index("col")
    p = 1 - c
    half, size = q.shape
    rmax = u.shape[0]
    params = d.shape[0]
    count = probes_ref.shape[0]
    pad = src_all.shape[1]
    group = m_all.shape[0]
    groups = lin_all.shape[0]
    g, l = i // group, i % group

    loads = [
        pltpu.make_async_copy(u_hbm.at[0], u, load_sem.at[0]),
        pltpu.make_async_copy(q_hbm.at[0], q, load_sem.at[1]),
        pltpu.make_async_copy(du_hbm.at[:, 0], du, load_sem.at[2]),
        pltpu.make_async_copy(dv_hbm.at[:, 0], dv, load_sem.at[3]),
        pltpu.make_async_copy(d_hbm.at[:, 0], d, load_sem.at[4]),
    ]
    own_v_load = pltpu.make_async_copy(v_hbm.at[0], own_v, load_sem.at[5])
    small_loads = [
        pltpu.make_async_copy(probes_hbm, probes_ref, load_sem.at[6]),
        pltpu.make_async_copy(white_hbm, white_ref, load_sem.at[7]),
        pltpu.make_async_copy(ranks_hbm, ranks_ref, load_sem.at[8]),
    ]
    own_v_load.start()
    for load in small_loads:
        load.start()
    for load in loads:
        load.start()

    barrier = pltpu.get_barrier_semaphore()

    def greet(row, col):
        pl.semaphore_signal(barrier, inc=1, device_id=(row, col), device_id_type=MESH)

    from_above, to_below = jnp.logical_and(l == 0, i > 0), jnp.logical_and(l == group - 1, i < rows - 1)
    greet(i, p)
    for k in range(1, group):
        greet(g * group + lax.rem(l + k, group), c)

    @pl.when(from_above)
    def _():
        greet(i - 1, c)

    @pl.when(to_below)
    def _():
        greet(i + 1, c)

    for k in range(1, groups):
        greet(lax.rem(g + k, groups) * group + l, c)
    pl.semaphore_wait(
        barrier, group + groups - 1 + from_above.astype(jnp.int32) + to_below.astype(jnp.int32)
    )

    def pair(k, src, dst):
        return pltpu.make_async_remote_copy(
            src_ref=src, dst_ref=dst, send_sem=pair_send.at[k], recv_sem=pair_recv.at[k],
            device_id=(i, p), device_id_type=MESH,
        )

    def hop(sent, k, src, dst, distance):
        return pltpu.make_async_remote_copy(
            src_ref=src, dst_ref=dst, send_sem=row_send.at[sent], recv_sem=row_recv.at[k],
            device_id=(lax.rem(i + distance + rows, rows), c), device_id_type=MESH,
        )

    def halves_of(block):
        low, high = block[:, :half], block[:, half:]
        return jnp.where(c == 0, low, high), jnp.where(c == 0, high, low)

    own_v_load.wait()
    v_hop = hop(0, 0, own_v, v_all.at[c], -1)

    @pl.when(i > 0)
    def _():
        v_hop.start()

    for load in small_loads:
        load.wait()
    signs = probes_ref[...].astype(f32)
    src_own = jnp.concatenate(
        [signs, white_ref[...].reshape(1, half), jnp.zeros((pad - count - 1, half), f32)], axis=0
    )
    src_all[c] = src_own
    src_pair = pair(0, src_all.at[c], src_all.at[c])
    src_pair.start()

    row_of = lax.broadcasted_iota(jnp.int32, (rmax, 1), 0)
    loads[0].wait()
    u_split = split(u[...] * (row_of < ranks_ref[:, 0:1]).astype(f32))
    loads[1].wait()
    q_high[...], q_low[...] = split(q[...])
    p_own, p_send[...] = halves_of(dot3(u_split, (q_high[...], q_low[...]), NN))
    p_pair = pair(1, p_send, p_recv)
    p_pair.start()
    for load in loads[2:4]:
        load.wait()
    for k in range(params):
        du_high[k], du_low[k] = split(du[k] * (row_of < ranks_ref[:, k + 1:k + 2]).astype(f32))
        dv_high[k], dv_low[k] = split(dv[k])
    p_pair.wait_recv()
    p_high[...], p_low[...] = split(p_own + p_recv[...])
    src_pair.wait_recv()

    v_pair = pair(2, v_all.at[c], v_all.at[c])

    @pl.when(i < rows - 1)
    def _():
        v_hop.wait_recv()

    @pl.when(i == rows - 1)
    def _():
        v_all[c] = jnp.zeros((rmax, half), f32)

    v_pair.start()
    p_split = (p_high[...], p_low[...])
    m_part[...] = dot3(split(jnp.concatenate([v_all[c], src_own], axis=0)), p_split, NT)
    m_pair = pair(3, m_part, m_other)
    m_pair.start()
    m_pair.wait_recv()
    m_all[l] = m_part[...] + m_other[...]

    def drain(block, number, sem):
        blocks = block.at[pl.ds(0, number)]
        pltpu.make_async_copy(blocks, blocks, sem).wait()

    in_group = lambda member: g * group + member
    across = lambda other: other * group + l

    for k in range(1, group):
        pltpu.make_async_remote_copy(
            src_ref=m_all.at[l], dst_ref=m_all.at[l], send_sem=g1_send.at[0], recv_sem=g1_recv.at[0],
            device_id=(in_group(lax.rem(l + k, group)), c), device_id_type=MESH,
        ).start()

    v_pair.wait_recv()
    halves = [jnp.concatenate([v_all[s], src_all[s]], axis=0) for s in range(2)]
    both = dot3(split(jnp.concatenate(halves, axis=1)), (q_high[...], q_low[...]), NT)
    base = both[rmax:]
    both_split = split(both)
    wide_split = tuple(part[:rmax] for part in both_split)
    du_split = [(du_high[k], du_low[k]) for k in range(params)]
    dv_split = [(dv_high[k], dv_low[k]) for k in range(params)]
    for k in range(params):
        wd_part[k] = dot3(both_split, du_split[k], NT)
    wd_pair = pair(4, wd_part, wd_other)
    wd_pair.start()

    drain(m_all, group - 1, g1_recv.at[0])
    m_split = [split(m_all[m, :rmax]) for m in range(group)]
    lift = [m_all[m, rmax:] for m in range(group)]
    lin, off = -m_all[group - 1, :rmax], lift[group - 1]
    own_lin, own_off = lin, off
    lin_split = {group - 1: split(lin)}
    for m in reversed(range(group - 1)):
        own_lin, own_off = jnp.where(l <= m, lin, own_lin), jnp.where(l <= m, off, own_off)
        off_split = split(off)
        state = dot3(
            tuple(jnp.concatenate(part, axis=0) for part in zip(lin_split[m + 1], off_split)), m_split[m], NN
        )
        lin, off = -state[:rmax], lift[m] - state[rmax:]
        if m > 0:
            lin_split[m] = split(lin)
    lin_all[g] = lin
    off_all[g] = off

    def to_groups(block, send, recv, into):
        return [
            pltpu.make_async_remote_copy(
                src_ref=block.at[g], dst_ref=into.at[g],
                send_sem=send.at[m], recv_sem=recv.at[g],
                device_id=(across(m), c), device_id_type=MESH,
            )
            for m in range(groups)
        ]

    def from_group(block, recv, m):
        return pltpu.make_async_remote_copy(
            src_ref=block.at[m], dst_ref=block.at[m],
            send_sem=recv.at[m], recv_sem=recv.at[m],
            device_id=(across(m), c), device_id_type=MESH,
        )

    def when_each(test, act, items):
        for m, item in enumerate(items):
            @pl.when(test(m))
            def _():
                act(item)

    everyone = list(range(groups))
    inner = jnp.logical_and(g > 0, g < groups - 1)
    lin_back = to_groups(lin_all, l_send, l_recv, lin_all)
    lin_on = to_groups(lin_all, l_send, l_recv, lin_ahead)
    off_copies = to_groups(off_all, g2_send, g2_recv, off_all)
    when_each(lambda m: m < g, lambda copy: copy.start(), off_copies)
    when_each(lambda m: jnp.logical_and(inner, m < g), lambda copy: copy.start(), lin_back)
    when_each(lambda m: jnp.logical_and(inner, m > g), lambda copy: copy.start(), lin_on)

    own_lin_split = split(own_lin)
    lead = -m_all[0, :rmax]
    own_lead = lead
    for m in range(1, group - 1):
        lead = -dot3(m_split[m], split(lead), NN)
        own_lead = jnp.where(l > m, lead, own_lead)
    lead_split = split(own_lead)
    wd_pair.wait_recv()
    up_base, dvw_split = [], []
    for k in range(params):
        wd = wd_part[k] + wd_other[k]
        expanded = dot3(split(wd), dv_split[k], NN)
        dvw_split.append(split(expanded[:rmax]))
        up_base.append(expanded[rmax:])

    maps = everyone[1:groups - 1]
    when_each(lambda m: m > g, lambda m: from_group(off_all, g2_recv, m).wait_recv(), everyone)
    when_each(lambda k: maps[k] > g, lambda m: from_group(lin_all, l_recv, m).wait_recv(), maps)
    t_split = [split(lin_all[m]) for m in range(groups)]
    a = jnp.zeros((pad, rmax), f32)
    for m in reversed(range(1, groups)):
        new = off_all[m]
        if m < groups - 1:
            new = new + dot3(split(a), t_split[m], NN)
        a = jnp.where(m > g, new, a)
    a = jnp.where(l < group - 1, own_off + dot3(split(a), own_lin_split, NN), a)

    a_split = split(a)
    x = base - dot3(a_split, wide_split, NN)
    x_own[...] = x

    def pieces(sent, first, src, dst, distance):
        return [
            hop(sent, first + k, src.at[pl.ds(k * 8, 8)], dst.at[pl.ds(k * 8, 8)], distance)
            for k in range(src.shape[0] // 8)
        ]

    x_hops = pieces(1, 1, x_own, x_prior, 1)
    up_hops = pieces(2, 1 + pad // 8, up_send, up_recv, -1)

    def start_when(test, copies):
        @pl.when(test)
        def _():
            for copy in copies:
                copy.start()

    start_when(i < rows - 1, x_hops[:count // 8])

    def pack(ref, k, block):
        ref[k * count:(k + 1) * count] = block[:count]
        ref[params * count + k:params * count + k + 1] = block[count:count + 1]

    for k in range(params):
        pack(up_send, k, up_base[k] - dot3(a_split, dvw_split[k], NN))
        start_when(i > 0, up_hops[k * count // 8:(k + 1) * count // 8])
    start_when(i < rows - 1, x_hops[count // 8:])
    start_when(i > 0, up_hops[params * count // 8:])

    solved_ref[0:1] = x[count:count + 1]
    solved_ref[1:] = x[:count]
    rounded = x.astype(bf16)
    loads[4].wait()
    for k in range(params):
        mine, theirs = halves_of(dot1(rounded, d[k], NN))
        pack(dense_own, k, mine)
        pack(dense_send, k, theirs)
    dense_pair = pair(5, dense_send, dense_recv)
    dense_pair.start()

    def wait_or_clear(test, copies, rows_of):
        @pl.when(test)
        def _():
            for copy in copies:
                copy.wait_recv()

        @pl.when(jnp.logical_not(test))
        def _():
            rows_of[...] = jnp.zeros(rows_of.shape, f32)

    wait_or_clear(i > 0, x_hops[:count // 8], x_prior.at[pl.ds(0, count)])
    signs_split = split(x_prior[:count])
    s_low = jnp.concatenate([dot3(signs_split, dvw_split[k], NT) for k in range(params)], axis=0)
    dense_pair.wait_recv()
    probe_rows = params * count
    wait_or_clear(i < rows - 1, up_hops[:probe_rows // 8], up_recv.at[pl.ds(0, probe_rows)])

    applied = dense_own[:probe_rows] + dense_recv[:probe_rows] + up_recv[:probe_rows]
    s_all[2 * l + c] = dot3(split(applied), wide_split, NT) + s_low
    for k in range(group):
        for other in range(2):
            if k > 0 or other > 0:
                pltpu.make_async_remote_copy(
                    src_ref=s_all.at[2 * l + c], dst_ref=s_all.at[2 * l + c],
                    send_sem=g3_send.at[0], recv_sem=g3_recv.at[0],
                    device_id=(in_group(lax.rem(l + k, group)), (c, p)[other]), device_id_type=MESH,
                ).start()

    rest = x_prior.shape[0] - count
    wait_or_clear(i > 0, x_hops[count // 8:], x_prior.at[pl.ds(count, rest)])
    prior_split = split(x_prior[...])
    for k in range(params):
        low_part[k] = dot3(prior_split, dv_split[k], NT)
    low_pair = pair(6, low_part, low_other)
    low_pair.start()
    rest = up_recv.shape[0] - probe_rows
    wait_or_clear(i < rows - 1, up_hops[probe_rows // 8:], up_recv.at[pl.ds(probe_rows, rest)])
    low_pair.wait_recv()
    lower = [dot3(split(low_part[k] + low_other[k]), du_split[k], NN) for k in range(params)]
    drive = applied + jnp.concatenate([block[:count] for block in lower], axis=0)
    white_rows = pl.ds(probe_rows, params)
    seen = dense_own[white_rows] + dense_recv[white_rows] + up_recv[white_rows]
    observed = [seen[k:k + 1] + lower[k][count:count + 1] for k in range(params)]
    w, w_send[...] = halves_of(dot3(split(drive), (q_high[...], q_low[...]), NN))
    w_pair = pair(7, w_send, w_recv)
    w_pair.start()

    drain(s_all, 2 * group - 1, g3_recv.at[0])
    s_sum = [s_all[2 * m] + s_all[2 * m + 1] for m in range(group)]
    s_split = [split(s_sum[m]) for m in range(group - 1)]
    total = s_sum[group - 1]
    for m in range(group - 1):
        total = total + dot3(s_split[m], lin_split[m + 1], NT)
    o_all[g] = total
    o_copies = to_groups(o_all, g4_send, g4_recv, o_all)
    when_each(lambda m: m > g, lambda copy: copy.start(), o_copies)
    b = jnp.where(l > 0, s_sum[0], 0.0)
    for m in range(1, group - 1):
        b = jnp.where(m < l, s_sum[m] - dot3(split(b), m_split[m], NT), b)
    w_pair.wait_recv()
    w = w + w_recv[...] - dot3(split(b), p_split, NN)
    when_each(lambda k: maps[k] < g, lambda m: from_group(lin_ahead, l_recv, m).wait_recv(), maps)
    when_each(lambda m: m < g, lambda m: from_group(o_all, g4_recv, m).wait_recv(), everyone)
    b = jnp.zeros((params * count, rmax), f32)
    for m in range(groups - 1):
        new = o_all[m]
        if m > 0:
            new = new + dot3(split(b), split(lin_ahead[m]), NT)
        b = jnp.where(m < g, new, b)
    b = jnp.where(l > 0, dot3(split(b), lead_split, NT), b)

    w = w - dot3(split(b), p_split, NN)
    parts = [w[k * count:(k + 1) * count] for k in range(params)]
    for k in range(params):
        deriv_ref[k] = parts[k]

    lanes = tot_all.shape[2]
    lane = lax.broadcasted_iota(jnp.int32, (1, lanes), 1)
    packed = jnp.zeros((1, lanes), f32)

    def put(packed, at, value):
        summed = jnp.sum(jnp.sum(value, axis=0, keepdims=True), axis=1, keepdims=True)
        return jnp.where(lane == at, summed, packed)

    for k in range(params):
        for m in range(k, params):
            product = parts[k] * parts[m]
            packed = put(packed, k * params + m, product)
        packed = put(packed, params * params + k, parts[k] * signs)
        data = observed[k] * x[count:count + 1]
        packed = put(packed, params * params + params + k, data)
    me = 2 * i + c
    devices = 2 * rows
    tot_all[me] = packed

    def tot_start(k, carry):
        other = lax.rem(me + k, devices)
        pltpu.make_async_remote_copy(
            src_ref=tot_all.at[me], dst_ref=tot_all.at[me], send_sem=tot_send.at[0], recv_sem=tot_recv.at[0],
            device_id=(other // 2, lax.rem(other, 2)), device_id_type=MESH,
        ).start()
        return carry

    lax.fori_loop(1, devices, tot_start, 0, unroll=min(devices - 1, 31))

    for copy in (src_pair, p_pair, v_pair, m_pair, wd_pair, dense_pair, low_pair, w_pair):
        copy.wait_send()
    drain(m_all, group - 1, g1_send.at[0])
    drain(s_all, 2 * group - 1, g3_send.at[0])
    when_each(lambda m: m < g, lambda copy: copy.wait_send(), off_copies)
    when_each(lambda m: jnp.logical_and(inner, m != g), lambda copy: copy.wait_send(), lin_back)
    when_each(lambda m: m > g, lambda copy: copy.wait_send(), o_copies)

    @pl.when(i > 0)
    def _():
        v_hop.wait_send()
        hop(2, 0, up_send, up_recv, -1).wait_send()

    @pl.when(i < rows - 1)
    def _():
        hop(1, 0, x_own, x_prior, 1).wait_send()

    drain(tot_all, devices - 1, tot_send.at[0])
    drain(tot_all, devices - 1, tot_recv.at[0])
    sums = jnp.sum(tot_all[...], axis=0)
    locations = rows * size
    for k in range(params):
        for m in range(params):
            at = min(k, m) * params + max(k, m)
            fisher_ref[k:k + 1, m:m + 1] = sums[:, at:at + 1] / (2.0 * count * locations)
    at = params * params
    trace, data = sums[:, at:at + params], sums[:, at + params:at + 2 * params]
    score_ref[...] = (data - trace / count) / (2.0 * locations)


def store(*refs):
    sem = refs[-1]
    copies = [pltpu.make_async_copy(refs[k], refs[k + 4], sem.at[k]) for k in range(4)]
    for copy in copies:
        copy.start()
    for copy in copies:
        copy.wait()


def body(
    inv_diag, low_left, low_right, deriv_diag, deriv_left, deriv_right, ranks, whitened, probes
):
    rows = lax.axis_size("row")
    _, size, half = inv_diag.shape
    rmax = low_left.shape[2]
    params = deriv_left.shape[0]
    count = probes.shape[0]
    pad = -(-(count + 1) // 8) * 8
    group = group_size(rows)
    groups = rows // group
    devices = 2 * rows
    lanes = -(-(params * params + 2 * params) // 128) * 128
    vm, dma = pltpu.VMEM, pltpu.SemaphoreType.DMA
    high = rmax + pad
    packed = -(-params * (count + 1) // 8) * 8
    hops = 1 + pad // 8 + packed // 8
    outs = pl.pallas_call(
        functools.partial(kernel, rows),
        out_shape=(
            vm((count + 1, half), f32), vm((params, count, half), f32),
            vm((params, params), f32), vm((1, params), f32),
        ),
        in_specs=[pl.BlockSpec(memory_space=pltpu.HBM)] * 9,
        out_specs=[pl.BlockSpec(memory_space=pltpu.VMEM)] * 4,
        scratch_shapes=[
            vm((1, params + 1), jnp.int32), vm((half,), f32), vm((count, half), jnp.int32),
            vm((half, size), f32), vm((rmax, half), f32), vm((rmax, half), f32),
            vm((params, half, size), bf16), vm((params, rmax, half), f32),
            vm((params, rmax, half), f32), vm((half, size), bf16), vm((half, size), bf16),
            vm((2, rmax, half), f32), vm((2, pad, half), f32),
            vm((params, rmax, half), bf16), vm((params, rmax, half), bf16),
            vm((params, rmax, half), bf16), vm((params, rmax, half), bf16),
            vm((rmax, half), f32), vm((rmax, half), f32), vm((rmax, half), bf16), vm((rmax, half), bf16),
            vm((params, high, rmax), f32), vm((params, high, rmax), f32),
            vm((high, rmax), f32), vm((high, rmax), f32), vm((group, high, rmax), f32),
            vm((groups, rmax, rmax), f32), vm((groups, rmax, rmax), f32), vm((groups, pad, rmax), f32),
            vm((pad, half), f32), vm((pad, half), f32),
            vm((packed, half), f32), vm((packed, half), f32),
            vm((packed, half), f32), vm((packed, half), f32), vm((packed, half), f32),
            vm((params, pad, rmax), f32), vm((params, pad, rmax), f32),
            vm((2 * group, params * count, rmax), f32), vm((groups, params * count, rmax), f32),
            vm((params * count, half), f32), vm((params * count, half), f32),
            vm((devices, 1, lanes), f32),
            dma((9,)), dma((8,)), dma((8,)), dma((3,)), dma((hops,)),
            dma((1,)), dma((1,)), dma((groups,)), dma((groups,)), dma((groups,)), dma((groups,)),
            dma((1,)), dma((1,)), dma((groups,)), dma((groups,)),
            dma((1,)), dma((1,)),
        ],
        compiler_params=pltpu.CompilerParams(
            collective_id=0, has_side_effects=True, vmem_limit_bytes=60 * 1024 * 1024
        ),
    )(
        *[jnp.swapaxes(x, -1, -2) for x in (
            inv_diag, low_left, low_right, deriv_diag, deriv_left, deriv_right, ranks
        )],
        whitened, probes,
    )
    outs = pl.pallas_call(
        store,
        out_shape=tuple(jax.ShapeDtypeStruct(x.shape, x.dtype) for x in outs),
        in_specs=[pl.BlockSpec(memory_space=pltpu.VMEM)] * 4,
        out_specs=[pl.BlockSpec(memory_space=pltpu.HBM)] * 4,
        scratch_shapes=[dma((4,))],
    )(*[pltpu.with_memory_space_constraint(x, pltpu.VMEM) for x in outs])
    return outs[0], outs[1], outs[2], outs[3][0]


def solution(mesh):
    return jax.shard_map(
        body,
        mesh=mesh,
        in_specs=(
            P("row", None, "col"),
            P("row", "col", None),
            P("row", "col", None),
            P(None, "row", None, "col"),
            P(None, "row", "col", None),
            P(None, "row", "col", None),
            P(None, "row"),
            P(("row", "col")),
            P(None, ("row", "col")),
        ),
        out_specs=(P(None, ("row", "col")), P(None, None, ("row", "col")), P(), P()),
        check_vma=False,
    )
```
